32 devices in a mesh: ctx: 8 (over z, x), head: 4 (over y, core).
Axes of the slice: x: 2, y: 2, z: 4, core: 2. Of those that a mesh axis runs over, the one named last changes fastest.
Arguments:
- queries: bfloat16 [2048, 32, 128], P('ctx', 'head'), may hold values from -20 to 20
- key_states: bfloat16 [2048, 4, 128], P('ctx', 'head'), may hold values from -20 to 20
- segment_ids: int32 [2048], P('ctx'), may hold values from 0 to 5, never falling along the last dimension, each value on 1 to 1280 neighbouring positions
Outputs:
- row_entropy: float32 [32, 2048], P('head', 'ctx')
- row_max: float32 [32, 2048], P('head', 'ctx')
- token_entropy: float32 [2048], P('ctx')
- head_entropy: float32 [32], P('head')
- head_peak: float32 [32], P('head')
The draws below stay inside these ranges and needn't reach their ends.
Inputs may be any that keep to these rules, and one draw needn't show every extreme that they name: `segment_ids`: segment numbers never fall along the sequence; a document holds at most 1280 tokens.
All inputs are finite; a program needn't handle non-finite values.
Results may differ from the reference program's by a relative error of at most 0.0003.
Values may be sent and summed in bfloat16 or wider, within the bound.
A program may use at most 64 MiB of HBM per device.

```python
import math
import jax
import jax.numpy as jnp
import numpy as np
from jax import lax

HEADS = 32
KV_HEADS = 4
HEAD_DIM = 128
TOKENS = 2048


def draw_queries(key, part):
    shape = (TOKENS, HEADS, HEAD_DIM)
    values = jax.random.truncated_normal(jax.random.fold_in(key, 1), -6.0, 6.0, shape, jnp.float32)
    return values.astype(jnp.bfloat16)


def draw_key_states(key, part):
    shape = (TOKENS, KV_HEADS, HEAD_DIM)
    values = jax.random.truncated_normal(jax.random.fold_in(key, 2), -6.0, 6.0, shape, jnp.float32)
    return values.astype(jnp.bfloat16)


def length_profile(number_of, total, limit, lean):
    weights = [(1 << 20) // math.isqrt(rank ** lean) + 1 for rank in range(2, number_of + 1)]
    surplus, holding = total - limit - (number_of - 1), [1] * (number_of - 1)
    while surplus > 0:
        candidates = [i for i in range(number_of - 1) if holding[i] < limit]
        pool, remaining = sum([weights[i] for i in candidates]), surplus
        for i in candidates:
            more = min(limit - holding[i], max(1, remaining * weights[i] // pool), surplus)
            holding[i] = holding[i] + more
            surplus = surplus - more
    return np.array([limit] + holding)


def ragged_sizes(own_key, count, total, most, skew):
    if count == 2:
        one = jax.random.randint(own_key, (), max(1, total - most), min(most, total - 1) + 1)
        return jnp.stack([one, total - one])
    tallies = jnp.asarray(length_profile(count, total, most, skew), jnp.int32)
    couples = (count - 1) // 2
    giver, taker = tallies[1:1 + 2 * couples:2], tallies[2:2 + 2 * couples:2]
    slack = jnp.minimum(giver - 1, most - taker)
    passed = jax.random.randint(jax.random.fold_in(own_key, 1), (couples,), 0, 1 << 20) % (slack + 1)
    tallies = tallies.at[1:1 + 2 * couples:2].set(giver - passed).at[2:2 + 2 * couples:2].set(taker + passed)
    return tallies[jax.random.permutation(jax.random.fold_in(own_key, 2), count)]


def setup_inputs(seed: int = 0) -> dict:
    streams_of = jax.random.split(jax.random.key(seed), 4)
    queries = draw_queries(jax.random.fold_in(streams_of[3], 71), 0)
    key_states = draw_key_states(jax.random.fold_in(streams_of[3], 71), 0)
    segment_ids = jnp.searchsorted(jnp.cumsum(ragged_sizes(streams_of[2], 6, TOKENS, TOKENS * 5 // 8, 2)), jnp.arange(TOKENS), side="right").astype(jnp.int32)
    return {"queries": queries, "key_states": key_states, "segment_ids": segment_ids}


NEG_FILL = -1.0e30


def reference(queries, key_states, segment_ids):
    per_kv = HEADS // KV_HEADS
    score_scale = HEAD_DIM ** -0.5
    row_block = min(512, TOKENS)
    key_pos = jnp.arange(TOKENS, dtype=jnp.int32)

    def per_head(head_number):
        head_keys = lax.dynamic_index_in_dim(key_states, head_number // per_kv, 1, keepdims=False)
        head_queries = lax.dynamic_index_in_dim(queries, head_number, 1, keepdims=False)

        def per_block(block_number):
            begin = (block_number * row_block).astype(jnp.int32)
            query_block = lax.dynamic_slice_in_dim(head_queries, begin, row_block, 0)
            query_seg = lax.dynamic_slice_in_dim(segment_ids, begin, row_block, 0)
            logits = jnp.dot(query_block, head_keys.T, preferred_element_type=jnp.float32) * score_scale
            query_pos = begin + jnp.arange(row_block, dtype=jnp.int32)
            visible = (key_pos[None, :] <= query_pos[:, None]) & (segment_ids[None, :] == query_seg[:, None])
            peak = jnp.max(jnp.where(visible, logits, NEG_FILL), axis=1)
            shifted = logits - peak[:, None]
            expo = jnp.where(visible, jnp.exp(shifted), 0.0)
            mass = jnp.sum(expo, axis=1)
            moment = jnp.sum(expo * shifted, axis=1)
            return jnp.log(mass) - moment / mass, peak

        entropy, peak = lax.map(per_block, jnp.arange(TOKENS // row_block, dtype=jnp.int32))
        return entropy.reshape(TOKENS), peak.reshape(TOKENS)

    row_entropy, row_max = lax.map(per_head, jnp.arange(HEADS, dtype=jnp.int32))
    token_entropy = jnp.sum(row_entropy, axis=0) / HEADS
    head_entropy = jnp.sum(row_entropy, axis=1) / TOKENS
    head_peak = jnp.max(row_max, axis=1)
    return (row_entropy, row_max, token_entropy, head_entropy, head_peak)
```

```python
from functools import partial

import jax
import jax.numpy as jnp
from jax import lax
from jax.experimental import pallas as pl
from jax.experimental.pallas import tpu as pltpu
from jax.sharding import PartitionSpec as P

HEADS = 32
MESH = pl.DeviceIdType.MESH
NEG = -1e30
LOG2E = 1.4426950408889634
LN2 = 0.6931471805599453


def kernel(
    ctx_n, head_n, reach, q_hbm, k_ref, seg_ref,
    ent_ref, max_ref, tok_ref, hent_ref, hpeak_ref,
    q_in, q_t, k_col, k_x, seg_col, seg_x, bias, peaks, totals, moments,
    tok_out, tok_in, stat_out, stat_in, q_sem, send_sem, recv_sem, tok_sem, stat_sem,
):
    rows, heads, dim = q_in.shape
    scale = dim ** (-0.5)
    to_log2 = scale * LOG2E
    c = lax.axis_index("ctx")
    h_me = lax.axis_index("head")
    groups = ctx_n // 2
    steps = reach // 2
    g = c // 2
    m = c % 2

    q_copy = pltpu.make_async_copy(q_hbm, q_in, q_sem)
    q_copy.start()

    barrier = pltpu.get_barrier_semaphore()
    for o in range(1, ctx_n):
        pl.semaphore_signal(barrier, 1, device_id={"ctx": lax.rem(c + o, ctx_n)}, device_id_type=MESH)
    for o in range(1, head_n):
        pl.semaphore_signal(barrier, 1, device_id={"head": lax.rem(h_me + o, head_n)}, device_id_type=MESH)
    pl.semaphore_wait(barrier, ctx_n + head_n - 2)

    def send(lane, slot, src, dst, target):
        keys = pltpu.make_async_remote_copy(
            src[0], dst[0], send_sem.at[lane, slot, 0], recv_sem.at[lane, slot, 0],
            device_id={"ctx": target}, device_id_type=MESH)
        segs = pltpu.make_async_remote_copy(
            src[1], dst[1], send_sem.at[lane, slot, 1], recv_sem.at[lane, slot, 1],
            device_id={"ctx": target}, device_id_type=MESH)
        return keys, segs

    own = (k_ref, seg_ref)

    def col(s):
        return (k_col.at[s], seg_col.at[s])

    def across(s):
        return (k_x.at[s], seg_x.at[s])

    def column_send(s):
        return send(0, s, own, col(s), jnp.minimum(g + s, groups - 1) * 2 + m)

    def own_across():
        return send(1, 0, own, across(0), c + 1 - 2 * m)

    def relay(s):
        return send(1, s, col(s), across(s), c + 1 - 2 * m)

    far = steps + 1

    def far_send():
        return send(1, far, own, across(far), jnp.minimum(g + far, groups - 1) * 2)

    def go(copies):
        for copy in copies:
            copy.start()

    def sent(copies):
        for copy in copies:
            copy.wait_send()

    def came(copies):
        for copy in copies:
            copy.wait_recv()

    def column_ok(s):
        return g + s < groups

    def relay_ok(s):
        return (s <= g) & ((m == 1) | (2 * s + 1 <= reach))

    def from_partner_ok(s):
        return (s <= g) & ((m == 0) | (2 * s + 1 <= reach))

    odd = reach % 2 == 1
    far_ok = (m == 1) & (g + far < groups)
    from_far_ok = (m == 0) & (far <= g)

    @pl.when(m == 0)
    def _():
        go(own_across())

    for s in range(1, steps + 1):
        @pl.when(column_ok(s))
        def _():
            go(column_send(s))
    if odd:
        @pl.when(far_ok)
        def _():
            go(far_send())

    q_copy.wait()
    q_t[...] = jnp.swapaxes(q_in[...].astype(jnp.float32), 0, 1).astype(jnp.bfloat16)

    seg_row = seg_ref[...]
    seg_cols = jnp.broadcast_to(seg_row.astype(jnp.float32), (128, rows)).T
    key_at = lax.broadcasted_iota(jnp.int32, (rows, rows), 0)
    row_at = lax.broadcasted_iota(jnp.int32, (rows, rows), 1)
    same = seg_cols[:, :1] == seg_row.astype(jnp.float32)
    bias[...] = jnp.where(same & (key_at <= row_at), 0.0, NEG)

    def block_of(keys, head):
        raw = lax.dot_general(
            keys[...], q_t[head], (((1,), (1,)), ((), ())), preferred_element_type=jnp.float32)
        raw = raw + bias[...]
        peak = jnp.max(raw, axis=0, keepdims=True)
        shifted = (raw - peak) * to_log2
        expo = jnp.exp2(shifted)
        return (peak, jnp.sum(expo, axis=0, keepdims=True),
                jnp.sum(expo * shifted, axis=0, keepdims=True))

    for head in range(heads):
        peak, total, moment = block_of(k_ref, head)
        at = pl.ds(head, 1)
        peaks[at, :] = peak
        totals[at, :] = total
        moments[at, :] = moment

    first_seg = seg_row[:, :1]

    def add_block(keys, segs):
        hidden = rows - jnp.sum((segs[...] == first_seg).astype(jnp.int32), axis=1, keepdims=True)
        at_key = lax.broadcasted_iota(jnp.int32, (rows, rows), 0)
        bias[...] = jnp.where((at_key >= hidden) & (seg_row == first_seg), 0.0, NEG)
        for head in range(heads):
            peak, total, moment = block_of(keys, head)
            at = pl.ds(head, 1)
            old = peaks[at, :]
            top = jnp.maximum(old, peak)
            down = (old - top) * to_log2
            fresh = (peak - top) * to_log2
            keep = jnp.exp2(down)
            take = jnp.exp2(fresh)
            held = totals[at, :]
            peaks[at, :] = top
            moments[at, :] = keep * (moments[at, :] + down * held) + take * (moment + fresh * total)
            totals[at, :] = held * keep + total * take

    @pl.loop(1, steps + 1)
    def _(s):
        @pl.when(s <= g)
        def _():
            came(column_send(s))

            @pl.when(relay_ok(s))
            def _():
                go(relay(s))

            add_block(k_col.at[s], seg_col.at[s])

    @pl.loop(0, far + 1 if odd else far)
    def _(s):
        near = (s <= steps) & from_partner_ok(s) & ((m == 1) | (s >= 1))
        distant = (s == far) & from_far_ok

        @pl.when(near | distant)
        def _():
            came(relay(s))
            add_block(k_x.at[s], seg_x.at[s])

    entropy = jnp.log(totals[...]) - moments[...] * LN2 / totals[...]
    tops = peaks[...] * scale
    tok_part = jnp.sum(entropy, axis=0, keepdims=True)
    diag = (lax.broadcasted_iota(jnp.int32, (heads, 128), 0)
            == lax.broadcasted_iota(jnp.int32, (heads, 128), 1))
    sums = jnp.sum(jnp.where(diag, jnp.sum(entropy, axis=1, keepdims=True), 0.0), axis=0, keepdims=True)
    highs = jnp.max(jnp.where(diag, jnp.max(tops, axis=1, keepdims=True), NEG), axis=0, keepdims=True)
    stat_out[0:1, :] = sums
    stat_out[1:2, :] = highs
    tok_out[...] = tok_part
    ent_ref[...] = entropy
    max_ref[...] = tops

    def stat_send(o):
        return pltpu.make_async_remote_copy(
            stat_out, stat_in.at[o], stat_sem.at[0, o], stat_sem.at[1, o],
            device_id={"ctx": lax.rem(c + o, ctx_n)}, device_id_type=MESH)

    def tok_send(o):
        return pltpu.make_async_remote_copy(
            tok_out, tok_in.at[o], tok_sem.at[0, o], tok_sem.at[1, o],
            device_id={"head": lax.rem(h_me + o, head_n)}, device_id_type=MESH)

    for o in range(1, ctx_n):
        stat_send(o).start()
    for o in range(1, head_n):
        tok_send(o).start()

    @pl.when(m == 0)
    def _():
        sent(own_across())

    for s in range(1, steps + 1):
        @pl.when(column_ok(s))
        def _():
            sent(column_send(s))

        @pl.when(relay_ok(s))
        def _():
            sent(relay(s))
    if odd:
        @pl.when(far_ok)
        def _():
            sent(far_send())

    for o in range(1, head_n):
        tok_send(o).wait()
        tok_part = tok_part + tok_in[o]
    tok_ref[...] = tok_part / HEADS
    for o in range(1, ctx_n):
        stat_send(o).wait()
        sums = sums + stat_in[o, 0:1, :]
        highs = jnp.maximum(highs, stat_in[o, 1:2, :])
    hent_ref[...] = (sums / (rows * ctx_n))[:, :heads]
    hpeak_ref[...] = highs[:, :heads]


def shards(ctx_n, head_n, queries, key_states, segment_ids):
    rows, heads, dim = queries.shape
    longest = rows * ctx_n * 5 // 8
    reach = min(ctx_n - 1, (longest - 1 + rows - 1) // rows)
    slots = reach // 2 + 2
    vmem = pl.BlockSpec(memory_space=pltpu.VMEM)
    f32 = jnp.float32
    dma = pltpu.SemaphoreType.DMA
    ent, top, tok, hent, hpeak = pl.pallas_call(
        partial(kernel, ctx_n, head_n, reach),
        out_shape=[
            jax.ShapeDtypeStruct((heads, rows), f32),
            jax.ShapeDtypeStruct((heads, rows), f32),
            jax.ShapeDtypeStruct((1, rows), f32),
            jax.ShapeDtypeStruct((1, heads), f32),
            jax.ShapeDtypeStruct((1, heads), f32),
        ],
        in_specs=[pl.BlockSpec(memory_space=pl.ANY), vmem, vmem],
        out_specs=[vmem] * 5,
        scratch_shapes=[
            pltpu.VMEM((rows, heads, dim), jnp.bfloat16),
            pltpu.VMEM((heads, rows, dim), jnp.bfloat16),
            pltpu.VMEM((slots, rows, dim), jnp.bfloat16),
            pltpu.VMEM((slots, rows, dim), jnp.bfloat16),
            pltpu.VMEM((slots, 1, rows), jnp.int32),
            pltpu.VMEM((slots, 1, rows), jnp.int32),
            pltpu.VMEM((rows, rows), f32),
            pltpu.VMEM((heads, rows), f32),
            pltpu.VMEM((heads, rows), f32),
            pltpu.VMEM((heads, rows), f32),
            pltpu.VMEM((1, rows), f32),
            pltpu.VMEM((head_n, 1, rows), f32),
            pltpu.VMEM((2, 128), f32),
            pltpu.VMEM((ctx_n, 2, 128), f32),
            dma(()),
            dma((2, slots, 2)),
            dma((2, slots, 2)),
            dma((2, head_n)),
            dma((2, ctx_n)),
        ],
        compiler_params=pltpu.CompilerParams(collective_id=0, has_side_effects=True),
    )(queries, key_states.reshape(rows, dim), segment_ids.reshape(1, rows))
    return (ent, top, tok.reshape(rows), hent.reshape(heads), hpeak.reshape(heads))


def solution(mesh):
    return jax.shard_map(
        partial(shards, mesh.shape["ctx"], mesh.shape["head"]),
        mesh=mesh,
        in_specs=(P("ctx", "head", None), P("ctx", "head", None), P("ctx")),
        out_specs=(P("head", "ctx"), P("head", "ctx"), P("ctx"), P("head"), P("head")),
        check_vma=False,
    )
```

```python
from functools import partial

import jax
import jax.numpy as jnp
from jax import lax
from jax.experimental import pallas as pl
from jax.experimental.pallas import tpu as pltpu
from jax.sharding import PartitionSpec as P

HEADS = 32
MESH = pl.DeviceIdType.MESH
NEG = -1e30
LOG2E = 1.4426950408889634
LN2 = 0.6931471805599453


def kernel(
    ctx_n, head_n, reach, q_hbm, k_ref, seg_ref,
    ent_ref, max_ref, tok_ref, hent_ref, hpeak_ref,
    q_in, q_t, k_col, k_x, seg_col, seg_x, bias, peaks, totals, moments,
    tok_out, tok_in, stat_out, stat_in, q_sem, send_sem, recv_sem, tok_sem, stat_sem,
    up_sem, down_sem, pair_sem, slant_sem,
):
    rows, heads, dim = q_in.shape
    scale = dim ** (-0.5)
    to_log2 = scale * LOG2E
    c = lax.axis_index("ctx")
    h_me = lax.axis_index("head")
    groups = ctx_n // 2
    g = c // 2
    m = c % 2

    q_copy = pltpu.make_async_copy(q_hbm, q_in, q_sem)
    q_copy.start()

    def ring(o):
        return {"ctx": jnp.clip(c + o, 0, ctx_n - 1)}

    partner = {"ctx": c + 1 - 2 * m}
    has_next = g + 1 < groups
    has_last = g > 0
    steps = reach // 2
    far = steps + 1
    odd = reach % 2 == 1

    def tell(sem, target):
        pl.semaphore_signal(sem, 1, device_id=target, device_id_type=MESH)

    barrier = pltpu.get_barrier_semaphore()
    tell(barrier, partner)
    for o in range(1, head_n):
        tell(barrier, {"head": lax.rem(h_me + o, head_n)})

    @pl.when(has_next)
    def _():
        tell(barrier, ring(2))

    @pl.when(has_last)
    def _():
        tell(barrier, ring(-2))

    pl.semaphore_wait(barrier, head_n + has_next.astype(jnp.int32) + has_last.astype(jnp.int32))

    def parts(lane, src_slot, dst_slot, src, dst, target):
        half = rows // 2
        pieces = (
            (src[1], dst[1]),
            (src[0].at[pl.ds(0, half), :], dst[0].at[pl.ds(0, half), :]),
            (src[0].at[pl.ds(half, half), :], dst[0].at[pl.ds(half, half), :]),
        )
        return [
            pltpu.make_async_remote_copy(
                source, place, send_sem.at[lane, src_slot, i], recv_sem.at[lane, dst_slot, i],
                device_id=target, device_id_type=MESH)
            for i, (source, place) in enumerate(pieces)
        ]

    own = (k_ref, seg_ref)

    def col(s):
        return (k_col.at[s], seg_col.at[s])

    def across(s):
        return (k_x.at[s], seg_x.at[s])

    def onward(s, src):
        return parts(0, s, s + 1, src, col(s + 1), ring(2))

    def cross(s, src):
        return parts(1, s, s, src, across(s), partner)

    def slant():
        return parts(1, far, far, col(steps), across(far), ring(1))

    def onward_ok(s):
        return has_next & (s <= g) & (s + 1 <= steps)

    def cross_ok(s):
        return (s <= g) & ((m == 1) | (2 * s + 1 <= reach)) & ((m == 0) | (s >= 1))

    def from_cross_ok(s):
        return (s <= g) & ((m == 0) | (2 * s + 1 <= reach)) & ((m == 1) | (s >= 1))

    slant_ok = has_next & (m == 1) & (steps <= g)
    from_slant_ok = (m == 0) & (far <= g)

    @pl.when(onward_ok(0))
    def _():
        for copy in onward(0, own):
            copy.start()

    @pl.when(cross_ok(0))
    def _():
        for copy in cross(0, own):
            copy.start()

    if odd:
        @pl.when((m == 1) & has_last)
        def _():
            tell(slant_sem, ring(-2))

    @pl.when(has_next & (g == 0))
    def _():
        tell(up_sem, ring(2))

    @pl.when(has_last & jnp.logical_not(has_next))
    def _():
        tell(down_sem, ring(-2))

    def pass_tokens(up_now, down_now):
        @pl.when(has_last & up_now)
        def _():
            pl.semaphore_wait(up_sem, 1)

            @pl.when(has_next)
            def _():
                tell(up_sem, ring(2))

        @pl.when(has_next & down_now)
        def _():
            pl.semaphore_wait(down_sem, 1)

            @pl.when(has_last)
            def _():
                tell(down_sem, ring(-2))

    q_copy.wait()
    q_t[...] = jnp.swapaxes(q_in[...].astype(jnp.float32), 0, 1).astype(jnp.bfloat16)

    seg_row = seg_ref[...]
    seg_cols = jnp.broadcast_to(seg_row.astype(jnp.float32), (128, rows)).T
    key_at = lax.broadcasted_iota(jnp.int32, (rows, rows), 0)
    row_at = lax.broadcasted_iota(jnp.int32, (rows, rows), 1)
    same = seg_cols[:, :1] == seg_row.astype(jnp.float32)
    bias[...] = jnp.where(same & (key_at <= row_at), 0.0, NEG)

    def block_of(keys, head):
        raw = lax.dot_general(
            keys[...], q_t[head], (((1,), (1,)), ((), ())), preferred_element_type=jnp.float32)
        raw = raw + bias[...]
        peak = jnp.max(raw, axis=0, keepdims=True)
        shifted = (raw - peak) * to_log2
        expo = jnp.exp2(shifted)
        return (peak, jnp.sum(expo, axis=0, keepdims=True),
                jnp.sum(expo * shifted, axis=0, keepdims=True))

    for head in range(heads):
        peak, total, moment = block_of(k_ref, head)
        at = pl.ds(head, 1)
        peaks[at, :] = peak
        totals[at, :] = total
        moments[at, :] = moment

    first_seg = seg_row[:, :1]

    def add_block(keys, segs):
        hidden = rows - jnp.sum((segs[...] == first_seg).astype(jnp.int32), axis=1, keepdims=True)
        at_key = lax.broadcasted_iota(jnp.int32, (rows, rows), 0)
        bias[...] = jnp.where((at_key >= hidden) & (seg_row == first_seg), 0.0, NEG)
        for head in range(heads):
            peak, total, moment = block_of(keys, head)
            at = pl.ds(head, 1)
            old = peaks[at, :]
            top = jnp.maximum(old, peak)
            down = (old - top) * to_log2
            fresh = (peak - top) * to_log2
            keep = jnp.exp2(down)
            take = jnp.exp2(fresh)
            held = totals[at, :]
            peaks[at, :] = top
            moments[at, :] = keep * (moments[at, :] + down * held) + take * (moment + fresh * total)
            totals[at, :] = held * keep + total * take

    if odd:
        @pl.when((m == 1) & has_next)
        def _():
            pl.semaphore_wait(slant_sem, 1)

    @pl.loop(1, steps + 1)
    def _(s):
        @pl.when(s <= g)
        def _():
            arriving = onward(s - 1, col(s - 1))
            forward = onward(s, col(s))
            sideways = cross(s, col(s))
            slanted = slant() if odd else []
            for i, copy in enumerate(arriving):
                copy.wait_recv()

                @pl.when(onward_ok(s))
                def _():
                    forward[i].start()

                @pl.when(cross_ok(s))
                def _():
                    sideways[i].start()

                if odd:
                    @pl.when(slant_ok & (s == steps))
                    def _():
                        slanted[i].start()

            add_block(k_col.at[s], seg_col.at[s])

        pass_tokens(g == s, groups - 1 - g == s)

    pass_tokens(g > steps, groups - 1 - g > steps)
    tell(pair_sem, partner)

    @pl.loop(0, far + 1 if odd else far)
    def _(s):
        @pl.when(((s <= steps) & from_cross_ok(s)) | ((s == far) & from_slant_ok))
        def _():
            for copy in cross(s, across(s)):
                copy.wait_recv()
            add_block(k_x.at[s], seg_x.at[s])

    pl.semaphore_wait(pair_sem, 1)

    entropy = jnp.log(totals[...]) - moments[...] * LN2 / totals[...]
    tops = peaks[...] * scale
    tok_part = jnp.sum(entropy, axis=0, keepdims=True)
    diag = (lax.broadcasted_iota(jnp.int32, (heads, 128), 0)
            == lax.broadcasted_iota(jnp.int32, (heads, 128), 1))
    sums = jnp.sum(jnp.where(diag, jnp.sum(entropy, axis=1, keepdims=True), 0.0), axis=0, keepdims=True)
    highs = jnp.max(jnp.where(diag, jnp.max(tops, axis=1, keepdims=True), NEG), axis=0, keepdims=True)
    stat_out[0:1, :] = sums
    stat_out[1:2, :] = highs
    tok_out[...] = tok_part
    ent_ref[...] = entropy
    max_ref[...] = tops

    def stat_send(o):
        return pltpu.make_async_remote_copy(
            stat_out, stat_in.at[o], stat_sem.at[0, o], stat_sem.at[1, o],
            device_id={"ctx": lax.rem(c + o, ctx_n)}, device_id_type=MESH)

    def tok_send(o):
        return pltpu.make_async_remote_copy(
            tok_out, tok_in.at[o], tok_sem.at[0, o], tok_sem.at[1, o],
            device_id={"head": lax.rem(h_me + o, head_n)}, device_id_type=MESH)

    for o in range(1, ctx_n):
        stat_send(o).start()
    for o in range(1, head_n):
        tok_send(o).start()

    for s in range(steps + 1):
        @pl.when(onward_ok(s))
        def _():
            for copy in onward(s, own if s == 0 else col(s)):
                copy.wait_send()

        @pl.when(cross_ok(s))
        def _():
            for copy in cross(s, own if s == 0 else col(s)):
                copy.wait_send()
    if odd:
        @pl.when(slant_ok)
        def _():
            for copy in slant():
                copy.wait_send()

    for o in range(1, head_n):
        tok_send(o).wait()
        tok_part = tok_part + tok_in[o]
    tok_ref[...] = tok_part / HEADS
    for o in range(1, ctx_n):
        stat_send(o).wait()
        sums = sums + stat_in[o, 0:1, :]
        highs = jnp.maximum(highs, stat_in[o, 1:2, :])
    hent_ref[...] = (sums / (rows * ctx_n))[:, :heads]
    hpeak_ref[...] = highs[:, :heads]


def write_out(*refs):
    half = len(refs) // 2
    for source, target in zip(refs[:half], refs[half:]):
        target[...] = source[...]


def shards(ctx_n, head_n, queries, key_states, segment_ids):
    rows, heads, dim = queries.shape
    longest = rows * ctx_n * 5 // 8
    reach = min(ctx_n - 1, (longest - 1 + rows - 1) // rows)
    slots = reach // 2 + 2
    vmem = pl.BlockSpec(memory_space=pltpu.VMEM)
    f32 = jnp.float32
    dma = pltpu.SemaphoreType.DMA
    ent, top, tok, hent, hpeak = pl.pallas_call(
        partial(kernel, ctx_n, head_n, reach),
        out_shape=[
            jax.ShapeDtypeStruct((heads, rows), f32),
            jax.ShapeDtypeStruct((heads, rows), f32),
            jax.ShapeDtypeStruct((1, rows), f32),
            jax.ShapeDtypeStruct((1, heads), f32),
            jax.ShapeDtypeStruct((1, heads), f32),
        ],
        in_specs=[pl.BlockSpec(memory_space=pl.ANY), vmem, vmem],
        out_specs=[vmem] * 5,
        scratch_shapes=[
            pltpu.VMEM((rows, heads, dim), jnp.bfloat16),
            pltpu.VMEM((heads, rows, dim), jnp.bfloat16),
            pltpu.VMEM((slots, rows, dim), jnp.bfloat16),
            pltpu.VMEM((slots, rows, dim), jnp.bfloat16),
            pltpu.VMEM((slots, 1, rows), jnp.int32),
            pltpu.VMEM((slots, 1, rows), jnp.int32),
            pltpu.VMEM((rows, rows), f32),
            pltpu.VMEM((heads, rows), f32),
            pltpu.VMEM((heads, rows), f32),
            pltpu.VMEM((heads, rows), f32),
            pltpu.VMEM((1, rows), f32),
            pltpu.VMEM((head_n, 1, rows), f32),
            pltpu.VMEM((2, 128), f32),
            pltpu.VMEM((ctx_n, 2, 128), f32),
            dma(()),
            dma((2, slots, 3)),
            dma((2, slots, 3)),
            dma((2, head_n)),
            dma((2, ctx_n)),
        ] + [pltpu.SemaphoreType.REGULAR] * 4,
        compiler_params=pltpu.CompilerParams(collective_id=0, has_side_effects=True),
    )(queries, key_states.reshape(rows, dim), segment_ids.reshape(1, rows))
    results = (ent, top, tok, hent, hpeak)
    ent, top, tok, hent, hpeak = pl.pallas_call(
        write_out,
        out_shape=[jax.ShapeDtypeStruct(a.shape, a.dtype) for a in results],
        in_specs=[vmem] * 5,
        out_specs=[vmem] * 5,
    )(*results)
    return (ent, top, tok.reshape(rows), hent.reshape(heads), hpeak.reshape(heads))


def solution(mesh):
    return jax.shard_map(
        partial(shards, mesh.shape["ctx"], mesh.shape["head"]),
        mesh=mesh,
        in_specs=(P("ctx", "head", None), P("ctx", "head", None), P("ctx")),
        out_specs=(P("head", "ctx"), P("head", "ctx"), P("ctx"), P("head"), P("head")),
        check_vma=False,
    )
```

```python
from functools import partial

import jax
import jax.numpy as jnp
from jax import lax
from jax.experimental import pallas as pl
from jax.experimental.pallas import tpu as pltpu
from jax.sharding import PartitionSpec as P

HEADS = 32
MESH = pl.DeviceIdType.MESH
NEG = -1e30
LOG2E = 1.4426950408889634
LN2 = 0.6931471805599453


def kernel(
    ctx_n, head_n, reach, q_hbm, k_hbm, seg_hbm,
    ent_ref, max_ref, tok_ref, hent_ref, hpeak_ref,
    k_ref, seg_ref, q_in, q_t, k_col, k_x, seg_col, seg_x, bias, peaks, totals, moments,
    tok_out, tok_in, stat_out, stat_in, q_sem, send_sem, recv_sem, tok_sem, stat_sem, k_sem,
    up_sem, down_sem, pair_sem, slant_sem,
):
    rows, heads, dim = q_in.shape
    scale = dim ** (-0.5)
    to_log2 = scale * LOG2E
    c = lax.axis_index("ctx")
    h_me = lax.axis_index("head")
    groups = ctx_n // 2
    g = c // 2
    m = c % 2

    q_copy = pltpu.make_async_copy(q_hbm, q_in, q_sem)
    key_copy = pltpu.make_async_copy(k_hbm, k_ref, k_sem.at[0])
    seg_copy = pltpu.make_async_copy(seg_hbm, seg_ref, k_sem.at[1])
    key_copy.start()
    seg_copy.start()
    q_copy.start()

    def ring(o):
        return {"ctx": jnp.clip(c + o, 0, ctx_n - 1)}

    partner = {"ctx": c + 1 - 2 * m}
    has_next = g + 1 < groups
    has_last = g > 0
    steps = reach // 2
    far = steps + 1
    odd = reach % 2 == 1

    def tell(sem, target):
        pl.semaphore_signal(sem, 1, device_id=target, device_id_type=MESH)

    barrier = pltpu.get_barrier_semaphore()
    tell(barrier, partner)
    for o in range(1, head_n):
        tell(barrier, {"head": lax.rem(h_me + o, head_n)})

    @pl.when(has_next)
    def _():
        tell(barrier, ring(2))

    @pl.when(has_last)
    def _():
        tell(barrier, ring(-2))

    pl.semaphore_wait(barrier, head_n + has_next.astype(jnp.int32) + has_last.astype(jnp.int32))

    key_copy.wait()
    seg_copy.wait()

    def parts(lane, src_slot, dst_slot, src, dst, target):
        half = rows // 2
        pieces = (
            (src[1], dst[1]),
            (src[0].at[pl.ds(0, half), :], dst[0].at[pl.ds(0, half), :]),
            (src[0].at[pl.ds(half, half), :], dst[0].at[pl.ds(half, half), :]),
        )
        return [
            pltpu.make_async_remote_copy(
                source, place, send_sem.at[lane, src_slot, i], recv_sem.at[lane, dst_slot, i],
                device_id=target, device_id_type=MESH)
            for i, (source, place) in enumerate(pieces)
        ]

    own = (k_ref, seg_ref)

    def col(s):
        return (k_col.at[s], seg_col.at[s])

    def across(s):
        return (k_x.at[s], seg_x.at[s])

    def onward(s, src):
        return parts(0, s, s + 1, src, col(s + 1), ring(2))

    def cross(s, src):
        return parts(1, s, s, src, across(s), partner)

    def slant():
        return parts(1, far, far, col(steps), across(far), ring(1))

    def onward_ok(s):
        return has_next & (s <= g) & (s + 1 <= steps)

    def cross_ok(s):
        return (s <= g) & ((m == 1) | (2 * s + 1 <= reach)) & ((m == 0) | (s >= 1))

    def from_cross_ok(s):
        return (s <= g) & ((m == 0) | (2 * s + 1 <= reach)) & ((m == 1) | (s >= 1))

    slant_ok = has_next & (m == 1) & (steps <= g)
    from_slant_ok = (m == 0) & (far <= g)

    @pl.when(onward_ok(0))
    def _():
        for copy in onward(0, own):
            copy.start()

    @pl.when(cross_ok(0))
    def _():
        for copy in cross(0, own):
            copy.start()

    if odd:
        @pl.when((m == 1) & has_last)
        def _():
            tell(slant_sem, ring(-2))

    @pl.when(has_next & (g == 0))
    def _():
        tell(up_sem, ring(2))

    @pl.when(has_last & jnp.logical_not(has_next))
    def _():
        tell(down_sem, ring(-2))

    def pass_tokens(up_now, down_now):
        @pl.when(has_last & up_now)
        def _():
            pl.semaphore_wait(up_sem, 1)

            @pl.when(has_next)
            def _():
                tell(up_sem, ring(2))

        @pl.when(has_next & down_now)
        def _():
            pl.semaphore_wait(down_sem, 1)

            @pl.when(has_last)
            def _():
                tell(down_sem, ring(-2))

    q_copy.wait()
    q_t[...] = jnp.swapaxes(q_in[...].astype(jnp.float32), 0, 1).astype(jnp.bfloat16)

    seg_row = seg_ref[...]
    seg_cols = jnp.broadcast_to(seg_row.astype(jnp.float32), (128, rows)).T
    key_at = lax.broadcasted_iota(jnp.int32, (rows, rows), 0)
    row_at = lax.broadcasted_iota(jnp.int32, (rows, rows), 1)
    same = seg_cols[:, :1] == seg_row.astype(jnp.float32)
    bias[...] = jnp.where(same & (key_at <= row_at), 0.0, NEG)

    def block_of(keys, head):
        raw = lax.dot_general(
            keys[...], q_t[head], (((1,), (1,)), ((), ())), preferred_element_type=jnp.float32)
        raw = raw + bias[...]
        peak = jnp.max(raw, axis=0, keepdims=True)
        shifted = (raw - peak) * to_log2
        expo = jnp.exp2(shifted)
        return (peak, jnp.sum(expo, axis=0, keepdims=True),
                jnp.sum(expo * shifted, axis=0, keepdims=True))

    for head in range(heads):
        peak, total, moment = block_of(k_ref, head)
        at = pl.ds(head, 1)
        peaks[at, :] = peak
        totals[at, :] = total
        moments[at, :] = moment

    first_seg = seg_row[:, :1]

    def add_block(keys, segs):
        hidden = rows - jnp.sum((segs[...] == first_seg).astype(jnp.int32), axis=1, keepdims=True)
        at_key = lax.broadcasted_iota(jnp.int32, (rows, rows), 0)
        bias[...] = jnp.where((at_key >= hidden) & (seg_row == first_seg), 0.0, NEG)
        for head in range(heads):
            peak, total, moment = block_of(keys, head)
            at = pl.ds(head, 1)
            old = peaks[at, :]
            top = jnp.maximum(old, peak)
            down = (old - top) * to_log2
            fresh = (peak - top) * to_log2
            keep = jnp.exp2(down)
            take = jnp.exp2(fresh)
            held = totals[at, :]
            peaks[at, :] = top
            moments[at, :] = keep * (moments[at, :] + down * held) + take * (moment + fresh * total)
            totals[at, :] = held * keep + total * take

    if odd:
        @pl.when((m == 1) & has_next)
        def _():
            pl.semaphore_wait(slant_sem, 1)

    @pl.loop(1, steps + 1)
    def _(s):
        @pl.when(s <= g)
        def _():
            arriving = onward(s - 1, col(s - 1))
            forward = onward(s, col(s))
            sideways = cross(s, col(s))
            slanted = slant() if odd else []
            for i, copy in enumerate(arriving):
                copy.wait_recv()

                @pl.when(onward_ok(s))
                def _():
                    forward[i].start()

                @pl.when(cross_ok(s))
                def _():
                    sideways[i].start()

                if odd:
                    @pl.when(slant_ok & (s == steps))
                    def _():
                        slanted[i].start()

            add_block(k_col.at[s], seg_col.at[s])

        pass_tokens(g == s, groups - 1 - g == s)

    pass_tokens(g > steps, groups - 1 - g > steps)
    tell(pair_sem, partner)

    @pl.loop(0, far + 1 if odd else far)
    def _(s):
        @pl.when(((s <= steps) & from_cross_ok(s)) | ((s == far) & from_slant_ok))
        def _():
            for copy in cross(s, across(s)):
                copy.wait_recv()
            add_block(k_x.at[s], seg_x.at[s])

    pl.semaphore_wait(pair_sem, 1)

    entropy = jnp.log(totals[...]) - moments[...] * LN2 / totals[...]
    tops = peaks[...] * scale
    tok_part = jnp.sum(entropy, axis=0, keepdims=True)
    diag = (lax.broadcasted_iota(jnp.int32, (heads, 128), 0)
            == lax.broadcasted_iota(jnp.int32, (heads, 128), 1))
    sums = jnp.sum(jnp.where(diag, jnp.sum(entropy, axis=1, keepdims=True), 0.0), axis=0, keepdims=True)
    highs = jnp.max(jnp.where(diag, jnp.max(tops, axis=1, keepdims=True), NEG), axis=0, keepdims=True)
    stat_out[0:1, :] = sums
    stat_out[1:2, :] = highs
    tok_out[...] = tok_part
    ent_ref[...] = entropy
    max_ref[...] = tops

    def stat_send(o):
        return pltpu.make_async_remote_copy(
            stat_out, stat_in.at[o], stat_sem.at[0, o], stat_sem.at[1, o],
            device_id={"ctx": lax.rem(c + o, ctx_n)}, device_id_type=MESH)

    def tok_send(o):
        return pltpu.make_async_remote_copy(
            tok_out, tok_in.at[o], tok_sem.at[0, o], tok_sem.at[1, o],
            device_id={"head": lax.rem(h_me + o, head_n)}, device_id_type=MESH)

    for o in range(1, ctx_n):
        stat_send(o).start()
    for o in range(1, head_n):
        tok_send(o).start()

    for s in range(steps + 1):
        @pl.when(onward_ok(s))
        def _():
            for copy in onward(s, own if s == 0 else col(s)):
                copy.wait_send()

        @pl.when(cross_ok(s))
        def _():
            for copy in cross(s, own if s == 0 else col(s)):
                copy.wait_send()
    if odd:
        @pl.when(slant_ok)
        def _():
            for copy in slant():
                copy.wait_send()

    for o in range(1, head_n):
        tok_send(o).wait()
        tok_part = tok_part + tok_in[o]
    tok_ref[...] = tok_part / HEADS
    for o in range(1, ctx_n):
        stat_send(o).wait()
        sums = sums + stat_in[o, 0:1, :]
        highs = jnp.maximum(highs, stat_in[o, 1:2, :])
    hent_ref[...] = (sums / (rows * ctx_n))[:, :heads]
    hpeak_ref[...] = highs[:, :heads]


def write_out(*refs):
    half = len(refs) // 2
    for source, target in zip(refs[:half], refs[half:]):
        target[...] = source[...]


def shards(ctx_n, head_n, queries, key_states, segment_ids):
    rows, heads, dim = queries.shape
    longest = rows * ctx_n * 5 // 8
    reach = min(ctx_n - 1, (longest - 1 + rows - 1) // rows)
    slots = reach // 2 + 2
    vmem = pl.BlockSpec(memory_space=pltpu.VMEM)
    f32 = jnp.float32
    dma = pltpu.SemaphoreType.DMA
    ent, top, tok, hent, hpeak = pl.pallas_call(
        partial(kernel, ctx_n, head_n, reach),
        out_shape=[
            pltpu.VMEM((heads, rows), f32),
            pltpu.VMEM((heads, rows), f32),
            pltpu.VMEM((1, rows), f32),
            pltpu.VMEM((1, heads), f32),
            pltpu.VMEM((1, heads), f32),
        ],
        in_specs=[pl.BlockSpec(memory_space=pl.ANY)] * 3,
        out_specs=[vmem] * 5,
        scratch_shapes=[
            pltpu.VMEM((rows, dim), jnp.bfloat16),
            pltpu.VMEM((1, rows), jnp.int32),
            pltpu.VMEM((rows, heads, dim), jnp.bfloat16),
            pltpu.VMEM((heads, rows, dim), jnp.bfloat16),
            pltpu.VMEM((slots, rows, dim), jnp.bfloat16),
            pltpu.VMEM((slots, rows, dim), jnp.bfloat16),
            pltpu.VMEM((slots, 1, rows), jnp.int32),
            pltpu.VMEM((slots, 1, rows), jnp.int32),
            pltpu.VMEM((rows, rows), f32),
            pltpu.VMEM((heads, rows), f32),
            pltpu.VMEM((heads, rows), f32),
            pltpu.VMEM((heads, rows), f32),
            pltpu.VMEM((1, rows), f32),
            pltpu.VMEM((head_n, 1, rows), f32),
            pltpu.VMEM((2, 128), f32),
            pltpu.VMEM((ctx_n, 2, 128), f32),
            dma(()),
            dma((2, slots, 3)),
            dma((2, slots, 3)),
            dma((2, head_n)),
            dma((2, ctx_n)),
            dma((2,)),
        ] + [pltpu.SemaphoreType.REGULAR] * 4,
        compiler_params=pltpu.CompilerParams(collective_id=0, has_side_effects=True),
    )(queries, key_states.reshape(rows, dim), segment_ids.reshape(1, rows))
    results = [pltpu.with_memory_space_constraint(a, pltpu.VMEM) for a in (ent, top, tok, hent, hpeak)]
    ent, top, tok, hent, hpeak = pl.pallas_call(
        write_out,
        out_shape=[jax.ShapeDtypeStruct(a.shape, a.dtype) for a in results],
        in_specs=[vmem] * 5,
        out_specs=[vmem] * 5,
    )(*results)
    return (ent, top, tok.reshape(rows), hent.reshape(heads), hpeak.reshape(heads))


def solution(mesh):
    return jax.shard_map(
        partial(shards, mesh.shape["ctx"], mesh.shape["head"]),
        mesh=mesh,
        in_specs=(P("ctx", "head", None), P("ctx", "head", None), P("ctx")),
        out_specs=(P("head", "ctx"), P("head", "ctx"), P("ctx"), P("head"), P("head")),
        check_vma=False,
    )
```

```python
from functools import partial

import jax
import jax.numpy as jnp
from jax import lax
from jax.experimental import pallas as pl
from jax.experimental.pallas import tpu as pltpu
from jax.sharding import PartitionSpec as P

HEADS = 32
MESH = pl.DeviceIdType.MESH
NEG = -1e30
LOG2E = 1.4426950408889634
LN2 = 0.6931471805599453


def kernel(
    ctx_n, head_n, reach, q_hbm, k_hbm, seg_hbm,
    ent_ref, max_ref, tok_ref, hent_ref, hpeak_ref,
    k_ref, seg_ref, q_in, q_t, k_col, k_x, seg_col, seg_x, bias, peaks, totals, moments,
    tok_out, tok_in, stat_out, stat_in, q_sem, send_sem, recv_sem, tok_sem, stat_sem, k_sem,
    up_sem, down_sem, pair_sem, slant_sem,
):
    rows, heads, dim = q_in.shape
    scale = dim ** (-0.5)
    to_log2 = scale * LOG2E
    c = lax.axis_index("ctx")
    h_me = lax.axis_index("head")
    groups = ctx_n // 2
    g = c // 2
    m = c % 2

    q_copy = pltpu.make_async_copy(q_hbm, q_in, q_sem)
    key_copy = pltpu.make_async_copy(k_hbm, k_ref, k_sem.at[0])
    seg_copy = pltpu.make_async_copy(seg_hbm, seg_ref, k_sem.at[1])
    key_copy.start()
    seg_copy.start()
    q_copy.start()

    def ring(o):
        return {"ctx": jnp.clip(c + o, 0, ctx_n - 1)}

    partner = {"ctx": c + 1 - 2 * m}
    has_next = g + 1 < groups
    has_last = g > 0
    steps = reach // 2
    far = steps + 1
    odd = reach % 2 == 1

    def tell(sem, target):
        pl.semaphore_signal(sem, 1, device_id=target, device_id_type=MESH)

    barrier = pltpu.get_barrier_semaphore()
    tell(barrier, partner)
    for o in range(1, head_n):
        tell(barrier, {"head": lax.rem(h_me + o, head_n)})

    @pl.when(has_next)
    def _():
        tell(barrier, ring(2))

    @pl.when(has_last)
    def _():
        tell(barrier, ring(-2))

    pl.semaphore_wait(barrier, head_n + has_next.astype(jnp.int32) + has_last.astype(jnp.int32))

    key_copy.wait()
    seg_copy.wait()

    def parts(lane, src_slot, dst_slot, src, dst, target):
        half = rows // 2
        pieces = (
            (src[1], dst[1]),
            (src[0].at[pl.ds(0, half), :], dst[0].at[pl.ds(0, half), :]),
            (src[0].at[pl.ds(half, half), :], dst[0].at[pl.ds(half, half), :]),
        )
        return [
            pltpu.make_async_remote_copy(
                source, place, send_sem.at[lane, src_slot, i], recv_sem.at[lane, dst_slot, i],
                device_id=target, device_id_type=MESH)
            for i, (source, place) in enumerate(pieces)
        ]

    own = (k_ref, seg_ref)

    def col(s):
        return (k_col.at[s], seg_col.at[s])

    def across(s):
        return (k_x.at[s], seg_x.at[s])

    def onward(s, src):
        return parts(0, s, s + 1, src, col(s + 1), ring(2))

    def cross(s, src):
        return parts(1, s, s, src, across(s), partner)

    def slant():
        return parts(1, far, far, col(steps), across(far), ring(1))

    def onward_ok(s):
        return has_next & (s <= g) & (s + 1 <= steps)

    def cross_ok(s):
        return (s <= g) & ((m == 1) | (2 * s + 1 <= reach)) & ((m == 0) | (s >= 1))

    def from_cross_ok(s):
        return (s <= g) & ((m == 0) | (2 * s + 1 <= reach)) & ((m == 1) | (s >= 1))

    slant_ok = has_next & (m == 1) & (steps <= g)
    from_slant_ok = (m == 0) & (far <= g)

    @pl.when(onward_ok(0))
    def _():
        for copy in onward(0, own):
            copy.start()

    @pl.when(cross_ok(0))
    def _():
        for copy in cross(0, own):
            copy.start()

    if odd:
        @pl.when((m == 1) & has_last)
        def _():
            tell(slant_sem, ring(-2))

    @pl.when(has_next & (g == 0))
    def _():
        tell(up_sem, ring(2))

    @pl.when(has_last & jnp.logical_not(has_next))
    def _():
        tell(down_sem, ring(-2))

    def pass_tokens(up_now, down_now):
        @pl.when(has_last & up_now)
        def _():
            pl.semaphore_wait(up_sem, 1)

            @pl.when(has_next)
            def _():
                tell(up_sem, ring(2))

        @pl.when(has_next & down_now)
        def _():
            pl.semaphore_wait(down_sem, 1)

            @pl.when(has_last)
            def _():
                tell(down_sem, ring(-2))

    q_copy.wait()
    q_t[...] = jnp.swapaxes(q_in[...].astype(jnp.float32), 0, 1).astype(jnp.bfloat16)

    seg_row = seg_ref[...]
    seg_cols = jnp.broadcast_to(seg_row.astype(jnp.float32), (128, rows)).T
    key_at = lax.broadcasted_iota(jnp.int32, (rows, rows), 0)
    row_at = lax.broadcasted_iota(jnp.int32, (rows, rows), 1)
    same = seg_cols[:, :1] == seg_row.astype(jnp.float32)
    bias[...] = jnp.where(same & (key_at <= row_at), 0.0, NEG)

    def block_of(keys, head):
        raw = lax.dot_general(
            keys[...], q_t[head], (((1,), (1,)), ((), ())), preferred_element_type=jnp.float32)
        raw = raw + bias[...]
        peak = jnp.max(raw, axis=0, keepdims=True)
        shifted = (raw - peak) * to_log2
        expo = jnp.exp2(shifted)
        return (peak, jnp.sum(expo, axis=0, keepdims=True),
                jnp.sum(expo * shifted, axis=0, keepdims=True))

    for head in range(heads):
        peak, total, moment = block_of(k_ref, head)
        at = pl.ds(head, 1)
        peaks[at, :] = peak
        totals[at, :] = total
        moments[at, :] = moment

    first_seg = seg_row[:, :1]

    def set_bias(segs):
        hidden = rows - jnp.sum((segs[...] == first_seg).astype(jnp.int32), axis=1, keepdims=True)
        at_key = lax.broadcasted_iota(jnp.int32, (rows, rows), 0)
        bias[...] = jnp.where((at_key >= hidden) & (seg_row == first_seg), 0.0, NEG)

    def add_block(keys):
        for head in range(heads):
            peak, total, moment = block_of(keys, head)
            at = pl.ds(head, 1)
            old = peaks[at, :]
            top = jnp.maximum(old, peak)
            down = (old - top) * to_log2
            fresh = (peak - top) * to_log2
            keep = jnp.exp2(down)
            take = jnp.exp2(fresh)
            held = totals[at, :]
            peaks[at, :] = top
            moments[at, :] = keep * (moments[at, :] + down * held) + take * (moment + fresh * total)
            totals[at, :] = held * keep + total * take

    if odd:
        @pl.when((m == 1) & has_next)
        def _():
            pl.semaphore_wait(slant_sem, 1)

    @pl.loop(1, steps + 1)
    def _(s):
        @pl.when(s <= g)
        def _():
            arriving = onward(s - 1, col(s - 1))
            forward = onward(s, col(s))
            sideways = cross(s, col(s))
            slanted = slant() if odd else []
            for i, copy in enumerate(arriving):
                copy.wait_recv()

                @pl.when(onward_ok(s))
                def _():
                    forward[i].start()

                @pl.when(cross_ok(s))
                def _():
                    sideways[i].start()

                if odd:
                    @pl.when(slant_ok & (s == steps))
                    def _():
                        slanted[i].start()

            set_bias(seg_col.at[s])
            add_block(k_col.at[s])

        pass_tokens(g == s, groups - 1 - g == s)

    pass_tokens(g > steps, groups - 1 - g > steps)
    tell(pair_sem, partner)

    @pl.loop(0, far + 1 if odd else far)
    def _(s):
        @pl.when(((s <= steps) & from_cross_ok(s)) | ((s == far) & from_slant_ok))
        def _():
            segs, *halves = cross(s, across(s))
            segs.wait_recv()
            set_bias(seg_x.at[s])
            for copy in halves:
                copy.wait_recv()
            add_block(k_x.at[s])

    pl.semaphore_wait(pair_sem, 1)

    entropy = jnp.log(totals[...]) - moments[...] * LN2 / totals[...]
    tops = peaks[...] * scale
    tok_part = jnp.sum(entropy, axis=0, keepdims=True)
    diag = (lax.broadcasted_iota(jnp.int32, (heads, 128), 0)
            == lax.broadcasted_iota(jnp.int32, (heads, 128), 1))
    sums = jnp.sum(jnp.where(diag, jnp.sum(entropy, axis=1, keepdims=True), 0.0), axis=0, keepdims=True)
    highs = jnp.max(jnp.where(diag, jnp.max(tops, axis=1, keepdims=True), NEG), axis=0, keepdims=True)
    stat_out[0:1, :] = sums
    stat_out[1:2, :] = highs
    tok_out[...] = tok_part
    ent_ref[...] = entropy
    max_ref[...] = tops

    def stat_send(o):
        return pltpu.make_async_remote_copy(
            stat_out, stat_in.at[o], stat_sem.at[0, o], stat_sem.at[1, o],
            device_id={"ctx": lax.rem(c + o, ctx_n)}, device_id_type=MESH)

    def tok_send(o):
        return pltpu.make_async_remote_copy(
            tok_out, tok_in.at[o], tok_sem.at[0, o], tok_sem.at[1, o],
            device_id={"head": lax.rem(h_me + o, head_n)}, device_id_type=MESH)

    for o in range(1, ctx_n):
        stat_send(o).start()
    for o in range(1, head_n):
        tok_send(o).start()

    for s in range(steps + 1):
        @pl.when(onward_ok(s))
        def _():
            for copy in onward(s, own if s == 0 else col(s)):
                copy.wait_send()

        @pl.when(cross_ok(s))
        def _():
            for copy in cross(s, own if s == 0 else col(s)):
                copy.wait_send()
    if odd:
        @pl.when(slant_ok)
        def _():
            for copy in slant():
                copy.wait_send()

    for o in range(1, head_n):
        tok_send(o).wait()
        tok_part = tok_part + tok_in[o]
    tok_ref[...] = tok_part / HEADS
    for o in range(1, ctx_n):
        stat_send(o).wait()
        sums = sums + stat_in[o, 0:1, :]
        highs = jnp.maximum(highs, stat_in[o, 1:2, :])
    hent_ref[...] = (sums / (rows * ctx_n))[:, :heads]
    hpeak_ref[...] = highs[:, :heads]


def write_out(*refs):
    half = len(refs) // 2
    for source, target in zip(refs[:half], refs[half:]):
        target[...] = source[...]


def shards(ctx_n, head_n, queries, key_states, segment_ids):
    rows, heads, dim = queries.shape
    longest = rows * ctx_n * 5 // 8
    reach = min(ctx_n - 1, (longest - 1 + rows - 1) // rows)
    slots = reach // 2 + 2
    vmem = pl.BlockSpec(memory_space=pltpu.VMEM)
    f32 = jnp.float32
    dma = pltpu.SemaphoreType.DMA
    ent, top, tok, hent, hpeak = pl.pallas_call(
        partial(kernel, ctx_n, head_n, reach),
        out_shape=[
            pltpu.VMEM((heads, rows), f32),
            pltpu.VMEM((heads, rows), f32),
            pltpu.VMEM((1, rows), f32),
            pltpu.VMEM((1, heads), f32),
            pltpu.VMEM((1, heads), f32),
        ],
        in_specs=[pl.BlockSpec(memory_space=pl.ANY)] * 3,
        out_specs=[vmem] * 5,
        scratch_shapes=[
            pltpu.VMEM((rows, dim), jnp.bfloat16),
            pltpu.VMEM((1, rows), jnp.int32),
            pltpu.VMEM((rows, heads, dim), jnp.bfloat16),
            pltpu.VMEM((heads, rows, dim), jnp.bfloat16),
            pltpu.VMEM((slots, rows, dim), jnp.bfloat16),
            pltpu.VMEM((slots, rows, dim), jnp.bfloat16),
            pltpu.VMEM((slots, 1, rows), jnp.int32),
            pltpu.VMEM((slots, 1, rows), jnp.int32),
            pltpu.VMEM((rows, rows), f32),
            pltpu.VMEM((heads, rows), f32),
            pltpu.VMEM((heads, rows), f32),
            pltpu.VMEM((heads, rows), f32),
            pltpu.VMEM((1, rows), f32),
            pltpu.VMEM((head_n, 1, rows), f32),
            pltpu.VMEM((2, 128), f32),
            pltpu.VMEM((ctx_n, 2, 128), f32),
            dma(()),
            dma((2, slots, 3)),
            dma((2, slots, 3)),
            dma((2, head_n)),
            dma((2, ctx_n)),
            dma((2,)),
        ] + [pltpu.SemaphoreType.REGULAR] * 4,
        compiler_params=pltpu.CompilerParams(collective_id=0, has_side_effects=True),
    )(queries, key_states.reshape(rows, dim), segment_ids.reshape(1, rows))
    results = [pltpu.with_memory_space_constraint(a, pltpu.VMEM) for a in (ent, top, tok, hent, hpeak)]
    ent, top, tok, hent, hpeak = pl.pallas_call(
        write_out,
        out_shape=[jax.ShapeDtypeStruct(a.shape, a.dtype) for a in results],
        in_specs=[vmem] * 5,
        out_specs=[vmem] * 5,
    )(*results)
    return (ent, top, tok.reshape(rows), hent.reshape(heads), hpeak.reshape(heads))


def solution(mesh):
    return jax.shard_map(
        partial(shards, mesh.shape["ctx"], mesh.shape["head"]),
        mesh=mesh,
        in_specs=(P("ctx", "head", None), P("ctx", "head", None), P("ctx")),
        out_specs=(P("head", "ctx"), P("head", "ctx"), P("ctx"), P("head"), P("head")),
        check_vma=False,
    )
```
